128 devices in a mesh: gx: 8 (over x, core), gy: 16 (over y, z).
Axes of the slice: x: 4, y: 4, z: 4, core: 2. Of those that a mesh axis runs over, the one named last changes fastest.
Arguments:
- log_crit: float32 [1024, 1024, 128], P('gx', 'gy'), may hold values from -4 to 4
- col_bins: int32 [1024, 1024, 4], P('gx', 'gy'), may hold values from 0 to 127
- rate_table: bfloat16 [128, 64], replicated, may hold values from 0.0039978027 to 0.059814453
- tile_mask: int32 [32, 32, 4], P('gx', 'gy'), may hold values from 0 to 1, as said below
- tile_route: int32 [32, 32, 4], P('gx', 'gy'), may hold values from 0 to 15, as said below
- filt_x: float32 [1024], replicated, may hold values from 0.1 to 1, as said below
- filt_y: float32 [1024], replicated, may hold values from 0.1 to 1, as said below
Outputs:
- recomb: float32 [1024, 1024, 128], P('gx', 'gy')
- smoothed: float32 [1024, 1024, 128], P('gx', 'gy')
- load: float32 [8, 16], P('gx', 'gy')
The draws below stay inside these ranges and needn't reach their ends.
Inputs may be any that keep to these rules, and one draw needn't show every extreme that they name: `tile_mask`: tiles form blocks of 4 x 2 x 4 (indices a // 4, b // 2); among the blocks with the same a // 4, some block has all 32 tiles active. `tile_route`: counting only tiles with tile_mask 1: among the blocks with the same a // 4 at most 16 active tiles share a route, and in every draw some such row of blocks gives every route exactly 16; at most 2 active tiles of one block share a route, and in every draw some block has 2 that do. filt_x[m] == filt_x[1024 - m] for 0 < m < 1024. filt_y[n] == filt_y[1024 - n] for 0 < n < 1024.
All inputs are finite; a program needn't handle non-finite values.
Results may differ from the reference program's by a relative error of at most 0.0003.
Values sent between devices are 32-bit elements; how exact they have to be, the bound alone decides.
A program may use at most 128 MiB of HBM per device.

```python
import math
import jax
import jax.numpy as jnp
from jax import lax

TE = 32
TX = 4
TY = 2
TZ = 4
BINS = 128
NODES = 64
RECV = 16
NX = 1024
NY = 1024
NZ = 128
N_GX = 8
N_GY = 16


def tile_plan(key):
    base_key = jax.random.fold_in(key, 11)
    k_count, k_busy, k_row, k_perm, k_spare = jax.random.split(base_key, 5)
    tiles_block = TX * TY * TZ
    half_tiles = tiles_block // 2
    quarter_tiles = tiles_block // 4
    pair_cap = tiles_block // N_GY
    counts = jax.random.randint(k_count, (N_GX, N_GY), quarter_tiles, half_tiles)
    busiest = jax.random.randint(k_busy, (N_GX,), 0, N_GY)
    full_row = jax.random.randint(k_row, (), 0, N_GX)
    column_ids = jnp.arange(N_GY)[None, :]
    counts = jnp.where(jnp.arange(N_GX)[:, None] == full_row, half_tiles, counts)
    counts = jnp.where(column_ids == busiest[:, None], tiles_block, counts)
    counts = jnp.where(column_ids == (busiest[:, None] + 1) % N_GY, 0, counts)
    perm_keys = jax.random.split(k_perm, N_GX * N_GY)
    tile_ranks = jax.vmap(lambda sub_key: jax.random.permutation(sub_key, tiles_block))(perm_keys).reshape(N_GX, N_GY, tiles_block)
    active = (tile_ranks < counts[:, :, None]).astype(jnp.int32)
    row_flags = active.reshape(N_GX, N_GY * tiles_block)
    before = jnp.cumsum(row_flags, axis=1) - row_flags
    chosen = (before // pair_cap % N_GY).reshape(N_GX, N_GY, tiles_block)
    spare_route = jax.random.randint(k_spare, (N_GX, N_GY, tiles_block), 0, N_GY)
    routes = jnp.where(active == 1, chosen, spare_route).astype(jnp.int32)
    return (lay_out(active), lay_out(routes))


def lay_out(values):
    shaped = values.reshape(N_GX, N_GY, TX, TY, TZ).transpose(0, 2, 1, 3, 4)
    return shaped.reshape(N_GX * TX, N_GY * TY, TZ)


def window_draw(key, length):
    half = length // 2 + 1
    values = jnp.exp(jax.random.uniform(key, (half,), jnp.float32, math.log(0.1), 0.0))
    indices = jnp.arange(length)
    folded = jnp.minimum(indices, length - indices)
    return values[folded].astype(jnp.float32)


def draw_tile_mask(key, part):
    return tile_plan(key)[0]


def draw_tile_route(key, part):
    return tile_plan(key)[1]


def draw_filt_x(key, part):
    return window_draw(jax.random.fold_in(key, 21), NX)


def draw_filt_y(key, part):
    return window_draw(jax.random.fold_in(key, 23), NY)


def plant(result, own_key, smallest, largest):
    place = [jax.random.randint(jax.random.fold_in(own_key, axis), (), 0, length) for axis, length in enumerate(result.shape)]
    widest = result.shape.index(max(result.shape))
    beside = place[:widest] + [(place[widest] + 1) % result.shape[widest]] + place[widest + 1:]
    return result.at[tuple(place)].set(smallest).at[tuple(beside)].set(largest)


def block_scale(stream_key, dims, shards, low, largest):
    loudness = 1.0
    for position, parts in shards:
        heights = jax.random.uniform(jax.random.fold_in(jax.random.fold_in(stream_key, 6), position), (parts,), jnp.float32, low / len(shards), largest / len(shards))
        loudness = loudness * jnp.repeat(jnp.exp(heights), dims[position] // parts).reshape((-1,) + (1,) * (len(dims) - 1 - position))
    return loudness


def normal_values(own_key, shape, scale, reach, cuts=(), kind=jnp.bfloat16):
    drawn = scale * jax.random.normal(own_key, shape, jnp.float32)
    if cuts:
        drawn = drawn * block_scale(own_key, shape, cuts, -0.22, 0.18)
    return jnp.clip(drawn, -reach, reach).astype(kind)


def setup_inputs(seed: int = 0) -> dict:
    key_of = jax.random.split(jax.random.key(seed), 8)
    return {
        "log_crit": normal_values(key_of[0], (NX, NY, NZ), 1.0, 4.0, ((0, 8), (1, 16)), jnp.float32),
        "col_bins": plant(jax.random.randint(key_of[1], (NX, NY, TZ), 0, BINS), jax.random.fold_in(key_of[1], 1), 0, BINS - 1).astype(jnp.int32),
        "rate_table": jnp.clip(jnp.exp(jax.random.uniform(key_of[2], (BINS, NODES), jnp.float32, math.log(0.0039978027), math.log(0.059814453))), 0.0039978027, 0.059814453).astype(jnp.bfloat16),
        "tile_mask": draw_tile_mask(jax.random.fold_in(key_of[7], 71), 0),
        "tile_route": draw_tile_route(jax.random.fold_in(key_of[7], 71), 0),
        "filt_x": draw_filt_x(jax.random.fold_in(key_of[7], 71), 0),
        "filt_y": draw_filt_y(jax.random.fold_in(key_of[7], 71), 0),
    }


steepness = 3.0


def reference(log_crit, col_bins, rate_table, tile_mask, tile_route, filt_x, filt_y):
    size_x, size_y, size_z = log_crit.shape
    rows_x = N_GX * TX
    rows_y = N_GY * TY
    tile_cells = log_crit.reshape(rows_x, TE, rows_y, TE, TZ, TE).transpose(0, 2, 4, 1, 3, 5).reshape(-1, TE, TE, TE)
    tile_bins = col_bins.reshape(rows_x, TE, rows_y, TE, TZ).transpose(0, 2, 4, 1, 3).reshape(-1, TE, TE)
    live_flags = tile_mask.reshape(-1)
    table_f32 = rate_table.astype(jnp.float32)
    node_grid = -2.5 + 5.0 * jnp.arange(NODES, dtype=jnp.float32) / (NODES - 1)

    def tile_value(operands):
        field, bin_cols, is_live = operands
        table_rows = table_f32[bin_cols]

        def active(unused):
            cutoff = jax.nn.sigmoid((field[..., None] - node_grid) * steepness)
            return jnp.sum(cutoff * table_rows[:, :, None, :], axis=-1)

        def quiet(unused):
            return jnp.zeros_like(field)

        return lax.cond(is_live == 1, active, quiet, 0)

    values = lax.map(tile_value, (tile_cells, tile_bins, live_flags))
    tile_mean = jnp.mean(values.reshape(values.shape[0], -1), axis=1).reshape(rows_x, rows_y, TZ)
    onehot = (tile_route[..., None] == jnp.arange(N_GY)).astype(jnp.float32)
    per_row = jnp.einsum('abt,abtg->ag', tile_mean.astype(jnp.float32), onehot)
    load = jnp.sum(per_row.reshape(N_GX, TX, N_GY), axis=1) / RECV
    recomb = values.reshape(rows_x, rows_y, TZ, TE, TE, TE).transpose(0, 3, 1, 4, 2, 5).reshape(size_x, size_y, size_z)
    gain_plane = filt_x[:, None, None] * filt_y[None, :, None]
    z_block = 16 if size_z % 16 == 0 else size_z
    blocks = recomb.reshape(size_x, size_y, size_z // z_block, z_block).transpose(2, 0, 1, 3)

    def smooth_block(block):
        spectrum = jnp.fft.fft2(block, axes=(0, 1))
        return jnp.real(jnp.fft.ifft2(spectrum * gain_plane, axes=(0, 1))).astype(jnp.float32)

    smoothed = lax.map(smooth_block, blocks).transpose(1, 2, 0, 3).reshape(size_x, size_y, size_z)
    return recomb, smoothed, load
```

```python
import functools
import math

import jax
import jax.numpy as jnp
import numpy as np
from jax import lax
from jax.experimental import pallas as pl
from jax.experimental.pallas import tpu as pltpu
from jax.sharding import PartitionSpec as P

VMEM = pltpu.VMEM


def pair_constants(nodes):
    half = nodes // 2
    q = -2.5 + 5.0 * np.arange(half) / (nodes - 1)
    g = np.exp(3.0 * q)
    return g, g + 1.0 / g


def pair_table(rate_table):
    nodes = rate_table.shape[1]
    g, _ = pair_constants(nodes)
    table = rate_table.astype(jnp.float32).T
    a = table[: nodes // 2]
    b = table[nodes // 2 :][::-1]
    g = jnp.asarray(g[:, None], jnp.float32)
    return jnp.concatenate([a + b, a / g + b * g], axis=0)


def column_integral(field, index_row, table_ref, coef_ref, sums):
    nodes = table_ref.shape[0]
    half = nodes // 2
    _, s = pair_constants(nodes)
    index = jnp.broadcast_to(index_row, (8, 128))
    for part in range(nodes // 8):
        rows = pl.ds(8 * part, 8)
        coef_ref[rows, :] = jnp.take_along_axis(
            table_ref[rows, :], index, axis=1, mode="promise_in_bounds"
        )
    w = jnp.exp(3.0 * field)
    v = w + jnp.exp(-3.0 * field)
    total = jnp.zeros_like(field)
    for k in range(half):
        r = pl.reciprocal(v + np.float32(s[k]), approx=False)
        total = total + (w * coef_ref[k : k + 1, :] + coef_ref[half + k : half + k + 1, :]) * r
    return total


def kernel_rows(filt):
    size = filt.shape[0]
    inner = 32
    outer = size // inner
    a = np.arange(outer)[:, None] * np.arange(outer)[None, :]
    small = 2.0 * np.pi * (a % outer) / outer
    b = np.arange(inner)[:, None] * np.arange(size)[None, :]
    big = 2.0 * np.pi * (b % size) / size
    grid = filt.reshape(outer, inner)
    dot = functools.partial(jnp.einsum, precision=lax.Precision.HIGHEST)
    real = dot("ab,ar->br", grid, jnp.asarray(np.cos(small), jnp.float32))
    imag = dot("ab,ar->br", grid, jnp.asarray(np.sin(small), jnp.float32))
    real = jnp.tile(real, (1, size // outer))
    imag = jnp.tile(imag, (1, size // outer))
    c = jnp.sum(
        real * jnp.asarray(np.cos(big), jnp.float32) - imag * jnp.asarray(np.sin(big), jnp.float32),
        axis=0,
    )
    return (c / size).reshape(size // 128, 128)


def split(x):
    high = x.astype(jnp.bfloat16)
    return high, (x - high.astype(jnp.float32)).astype(jnp.bfloat16)


def build_circulants(c_ref, mat_ref):
    shift = lax.rem(
        lax.broadcasted_iota(jnp.int32, (128, 128), 1)
        - lax.broadcasted_iota(jnp.int32, (128, 128), 0)
        + 128,
        128,
    )
    upper = lax.broadcasted_iota(jnp.int32, (128, 128), 1) >= lax.broadcasted_iota(
        jnp.int32, (128, 128), 0
    )
    rolled = []
    for m in range(8):
        row = jnp.broadcast_to(c_ref[m : m + 1, :], (8, 128))
        rolled.append(
            jnp.concatenate(
                [
                    jnp.take_along_axis(row, shift[8 * g : 8 * g + 8], axis=1, mode="promise_in_bounds")
                    for g in range(16)
                ],
                axis=0,
            )
        )
    blocks = [jnp.where(upper, rolled[(-d) % 8], rolled[(-d - 1) % 8]) for d in range(8)]
    for d in range(-3, 4):
        near, far = blocks[d % 8], blocks[(d + 4) % 8]
        for sign, value in enumerate((0.5 * (near + far), 0.5 * (near - far))):
            for part, piece in enumerate(split(value)):
                for i in range(4):
                    j = i - d
                    if 0 <= j < 4:
                        mat_ref[sign, part, pl.ds(128 * i, 128), pl.ds(128 * j, 128)] = piece


def dot3(a, b):
    d = functools.partial(jnp.dot, preferred_element_type=jnp.float32)
    return d(a[0], b[0]) + d(a[0], b[1]) + d(a[1], b[0])


MESH = pl.DeviceIdType.MESH


def fused_kernel(
    field_hbm, bins_ref, table_ref, mask_ref, route_ref, cx_ref, cy_ref,
    recomb_hbm, back_ref, share_ref,
    field_buf, out_buf, zsend_ref, recv_ref, mx_ref, my_ref, mid_ref, send_ref, give_ref,
    coef_ref, lt_ref, rt_ref, sum_ref,
    in_sem, out_sem, fsend_sem, frecv_sem, bsend_sem, brecv_sem, lsend_sem, lrecv_sem,
):
    n_gx, n_gy = lax.axis_size("gx"), lax.axis_size("gy")
    total = n_gx * n_gy
    gx, gy = lax.axis_index("gx"), lax.axis_index("gy")
    me = gx * n_gy + gy
    edge = 32
    layers = bins_ref.shape[1]
    chunks = zsend_ref.shape[0]
    pieces = send_ref.shape[0]
    piece_rows = send_ref.shape[2]

    def peer(k):
        offset = lax.rem(k * 37, total)
        return lax.rem(gx + offset // n_gy, n_gx), lax.rem(gy + lax.rem(offset, n_gy), n_gy)

    def forward(c, k):
        tx, ty = peer(k)
        return pltpu.make_async_remote_copy(
            src_ref=zsend_ref.at[c, tx * n_gy + ty], dst_ref=recv_ref.at[c, me],
            send_sem=fsend_sem.at[c], recv_sem=frecv_sem.at[c],
            device_id=(tx, ty), device_id_type=MESH,
        )

    def backward(p, k):
        tx, ty = peer(k)
        rows = pl.ds(pl.multiple_of(p * piece_rows, piece_rows), piece_rows)
        return pltpu.make_async_remote_copy(
            src_ref=send_ref.at[p, tx * n_gy + ty], dst_ref=back_ref.at[me, rows],
            send_sem=bsend_sem.at[p], recv_sem=brecv_sem.at[p],
            device_id=(tx, ty), device_id_type=MESH,
        )

    def load_copy(k):
        ty = lax.rem(gy + k, n_gy)
        return pltpu.make_async_remote_copy(
            src_ref=give_ref.at[ty], dst_ref=share_ref.at[gy],
            send_sem=lsend_sem, recv_sem=lrecv_sem,
            device_id=(gx, ty), device_id_type=MESH,
        )

    def fetch(c, slot):
        return pltpu.make_async_copy(
            field_hbm.at[:, pl.ds(pl.multiple_of(c * 8, 8), 8), :], field_buf.at[slot], in_sem.at[slot]
        )

    def put(c, slot):
        return pltpu.make_async_copy(
            out_buf.at[slot], recomb_hbm.at[:, pl.ds(pl.multiple_of(c * 8, 8), 8), :], out_sem.at[slot]
        )

    fetch(0, 0).start()
    barrier = pltpu.get_barrier_semaphore()

    def greet(k, _):
        tx, ty = peer(k)
        pl.semaphore_signal(barrier, inc=1, device_id=(tx, ty), device_id_type=MESH)
        return 0

    lax.fori_loop(1, total, greet, 0)
    sum_ref[...] = jnp.zeros_like(sum_ref)

    def evaluate_chunk(c, sending):
        slot = lax.rem(c, 2)

        @pl.when(c + 1 < chunks)
        def _():
            fetch(c + 1, 1 - slot).start()

        fetch(c, slot).wait()

        @pl.when(c >= 2)
        def _():
            put(c - 2, slot).wait()

        field2 = field_buf.at[slot].reshape(128 * 8, 128)
        out2 = out_buf.at[slot].reshape(128 * 8, 128)
        zsend2 = zsend_ref.at[c].reshape(128 * 8, 128)
        band = c * 8 // edge

        def per_row(y, _):
            lt_ref[...] = field2[pl.ds(y, 128, stride=8), :].T
            for t in range(layers):
                if sending:
                    per = total // 8 // layers
                    for s in range(per):
                        k = (y * layers + t) * per + s + 1
                        if t == layers - 1 and s == per - 1:
                            @pl.when(k < total)
                            def _():
                                forward(c - 1, k).start()
                        else:
                            forward(c - 1, k).start()
                z = pl.ds(edge * t, edge)
                value = column_integral(lt_ref[z, :], bins_ref[c * 8 + y, t : t + 1, :], table_ref, coef_ref, None)
                value = value * mask_ref[pl.ds(band * layers + t, 1), :]
                rt_ref[z, :] = value
                folded = (value[0:8] + value[8:16]) + (value[16:24] + value[24:32])
                sum_ref[band * layers + t] += folded
            zsend2[pl.ds(y, 128, stride=8), :] = rt_ref[...]
            out2[pl.ds(y, 128, stride=8), :] = rt_ref[...].T
            return 0

        lax.fori_loop(0, 8, per_row, 0)
        recv_ref[c, me] = zsend_ref[c, me]
        put(c, slot).start()

    evaluate_chunk(0, False)
    pl.semaphore_wait(barrier, total - 1)

    def later_chunk(c, _):
        evaluate_chunk(c, True)
        return 0

    lax.fori_loop(1, chunks, later_chunk, 0)

    def last_send(k, _):
        forward(chunks - 1, k).start()
        return 0

    lax.fori_loop(1, total, last_send, 0)

    flat = jnp.concatenate(
        [jnp.sum(sum_ref[i], axis=0, keepdims=True) for i in range(8)], axis=0
    )
    for g in range(16):
        give_ref[g] = jnp.where(route_ref[...] == g, flat, 0.0)
    share_ref[gy] = give_ref[gy]

    build_circulants(cx_ref, mx_ref)
    build_circulants(cy_ref, my_ref)

    def load_send(k, _):
        load_copy(k).start()
        return 0

    lax.fori_loop(1, n_gy, load_send, 0)

    def wait_all(ref, send_sem, recv_sem, what):
        copy = pltpu.make_async_remote_copy(
            src_ref=ref, dst_ref=ref, send_sem=send_sem, recv_sem=recv_sem,
            device_id=(gx, gy), device_id_type=MESH,
        )
        copy.wait_recv() if what == "recv" else copy.wait_send()

    def first(c, _):
        for q in range(2):
            wait_all(recv_ref.at[2 * c + q, pl.ds(0, total - 1)], fsend_sem.at[2 * c + q], frecv_sem.at[2 * c + q], "recv")

        def rows(i, j0):
            src = pl.ds(i * 16 + j0, 8)
            return jnp.concatenate([recv_ref[2 * c, src], recv_ref[2 * c + 1, src]], axis=1).reshape(128, 128)

        for ysign in range(2):
            parts = [[], []]
            for i in range(4):
                a0, a1 = rows(i, 0), rows(i, 8)
                b0, b1 = rows(i + 4, 0), rows(i + 4, 8)
                if ysign == 0:
                    a, b = a0 + a1, b0 + b1
                else:
                    a, b = a0 - a1, b0 - b1
                parts[0].append(a + b)
                parts[1].append(a - b)
            for xsign in range(2):
                value = split(jnp.concatenate(parts[xsign], axis=1))
                out = split(dot3(value, (mx_ref[xsign, 0], mx_ref[xsign, 1])))
                for part in range(2):
                    for j in range(8):
                        mid_ref[ysign, part, pl.ds(pl.multiple_of(64 * j + 16 * c, 16), 16), pl.ds(512 * xsign, 512)] = out[part][16 * j : 16 * j + 16]
        return 0

    lax.fori_loop(0, chunks // 2, first, 0)

    def second(p, _):
        res = []
        for ysign in range(2):
            mat = [
                jnp.concatenate(
                    [my_ref[ysign, part, pl.ds(pl.multiple_of(64 * j + 16 * p, 16), 16), :] for j in range(8)],
                    axis=0,
                )
                for part in range(2)
            ]
            res.append(dot3(mat, (mid_ref[ysign, 0], mid_ref[ysign, 1])))
        for yh in range(2):
            both = res[0] + res[1] if yh == 0 else res[0] - res[1]
            plus, minus = both[:, :512], both[:, 512:]
            for xh in range(2):
                value = plus + minus if xh == 0 else plus - minus
                for i in range(4):
                    for j in range(8):
                        send_ref[p, (xh * 4 + i) * 16 + yh * 8 + j] = value[16 * j : 16 * j + 16, 128 * i : 128 * i + 128]
        back_ref[me, pl.ds(pl.multiple_of(p * piece_rows, piece_rows), piece_rows)] = send_ref[p, me]

        def send(k, _):
            backward(p, k).start()
            return 0

        lax.fori_loop(1, total, send, 0)
        return 0

    lax.fori_loop(0, pieces, second, 0)

    def finish_forward(c, _):
        wait_all(zsend_ref.at[c, pl.ds(0, total - 1)], fsend_sem.at[c], frecv_sem.at[c], "send")
        return 0

    lax.fori_loop(0, chunks, finish_forward, 0)
    wait_all(share_ref.at[pl.ds(0, n_gy - 1)], lsend_sem, lrecv_sem, "recv")
    wait_all(give_ref.at[pl.ds(0, n_gy - 1)], lsend_sem, lrecv_sem, "send")
    put(chunks - 2, 0).wait()
    put(chunks - 1, 1).wait()

    def finish_backward(p, _):
        rows = pl.ds(pl.multiple_of(p * piece_rows, piece_rows), piece_rows)
        wait_all(back_ref.at[pl.ds(0, total - 1), rows], bsend_sem.at[p], brecv_sem.at[p], "recv")
        wait_all(send_ref.at[p, pl.ds(0, total - 1)], bsend_sem.at[p], brecv_sem.at[p], "send")
        return 0

    lax.fori_loop(0, pieces, finish_backward, 0)


def fused_call(log_crit, bins, table, mask_rows, route_rows, cx, cy):
    f32, bf16 = jnp.float32, jnp.bfloat16
    cells_x, cells_y, depth = log_crit.shape
    total = 128
    chunks, pieces = 8, 4
    dma, vmem, anywhere = pltpu.SemaphoreType.DMA, pl.BlockSpec(memory_space=VMEM), pl.BlockSpec(memory_space=pl.ANY)
    return pl.pallas_call(
        fused_kernel,
        in_specs=[anywhere] + [vmem] * 6,
        out_specs=[anywhere, vmem, vmem],
        out_shape=[
            jax.ShapeDtypeStruct((cells_x, cells_y, depth), f32),
            jax.ShapeDtypeStruct((total, cells_y, cells_x), f32),
            jax.ShapeDtypeStruct((16, 8, 128), f32),
        ],
        scratch_shapes=[
            VMEM((2, cells_x, 8, depth), f32),
            VMEM((2, cells_x, 8, depth), f32),
            VMEM((chunks, total, 8, 128), f32),
            VMEM((chunks, total, 8, 128), f32),
            VMEM((2, 2, 512, 512), bf16),
            VMEM((2, 2, 512, 512), bf16),
            VMEM((2, 2, 512, 1024), bf16),
            VMEM((pieces, total, 64 // pieces, 128), f32),
            VMEM((16, 8, 128), f32),
            VMEM(table.shape, f32),
            VMEM((128, 128), f32),
            VMEM((128, 128), f32),
            VMEM((8, 8, 128), f32),
            dma((2,)), dma((2,)), dma((chunks,)), dma((chunks,)), dma((pieces,)), dma((pieces,)), dma, dma,
        ],
        compiler_params=pltpu.CompilerParams(
            vmem_limit_bytes=60 * 2**20, collective_id=0, has_side_effects=True
        ),
        name="fused",
    )(log_crit, bins, table, mask_rows, route_rows, cx, cy)


def final_kernel(back_ref, recomb_ref, share_ref, out_ref, recomb_out, load_ref):
    source = back_ref.reshape(128 * 8, 128)
    target = out_ref.reshape(128 * 8, 128)
    for y in range(8):
        target[pl.ds(y, 128, stride=8), :] = source[pl.ds(y, 128, stride=8), :].T
    recomb_out[...] = recomb_ref[...]
    all_shares = jnp.sum(share_ref[...], axis=0)
    load_ref[...] = jnp.sum(jnp.sum(all_shares, axis=0, keepdims=True), axis=1, keepdims=True) * (2.0**-19)


def final_call(back, recomb, share):
    depth, cells_y, cells_x = back.shape
    steps = cells_y // 8
    f32 = jnp.float32
    slab = pl.BlockSpec((cells_x // steps, cells_y, depth), lambda c: (c, 0, 0))
    return pl.pallas_call(
        final_kernel,
        grid=(steps,),
        in_specs=[
            pl.BlockSpec((depth, 8, cells_x), lambda c: (0, c, 0)),
            slab,
            pl.BlockSpec(share.shape, lambda c: (0, 0, 0)),
        ],
        out_specs=[
            pl.BlockSpec((cells_x, 8, depth), lambda c: (0, c, 0)),
            slab,
            pl.BlockSpec((1, 1), lambda c: (0, 0)),
        ],
        out_shape=[
            jax.ShapeDtypeStruct((cells_x, cells_y, depth), f32),
            jax.ShapeDtypeStruct((cells_x, cells_y, depth), f32),
            jax.ShapeDtypeStruct((1, 1), f32),
        ],
        name="final",
    )(back, recomb, share)


def on_device(log_crit, col_bins, rate_table, tile_mask, tile_route, filt_x, filt_y):
    tiles_x = tile_mask.shape[0]
    edge = log_crit.shape[0] // tiles_x
    bins = col_bins.transpose(1, 2, 0)

    def rows_of(tiles):
        return jnp.repeat(tiles.transpose(1, 2, 0).reshape(-1, tiles_x), edge, axis=1)

    mask_rows = rows_of((tile_mask == 1).astype(jnp.float32))
    recomb, back, share = fused_call(
        log_crit, bins, pair_table(rate_table), mask_rows, rows_of(tile_route),
        kernel_rows(filt_x), kernel_rows(filt_y),
    )
    smoothed, recomb, load = final_call(back, recomb, share)
    return recomb, smoothed, load


def solution(mesh):
    block = P("gx", "gy", None)
    return jax.shard_map(
        on_device,
        mesh=mesh,
        in_specs=(block, block, P(), block, block, P(), P()),
        out_specs=(block, block, P("gx", "gy")),
        check_vma=False,
    )
```

```python
import functools

import jax
import jax.numpy as jnp
import numpy as np
from jax import lax
from jax.experimental import pallas as pl
from jax.experimental.pallas import tpu as pltpu
from jax.sharding import PartitionSpec as P

VMEM = pltpu.VMEM


MESH = pl.DeviceIdType.MESH
EDGE = 32


def pair_constants(nodes):
    half = nodes // 2
    q = -2.5 + 5.0 * np.arange(half) / (nodes - 1)
    g = np.exp(3.0 * q)
    return g, g + 1.0 / g


def wave_tables(size):
    inner = 32
    outer = size // inner
    a = np.arange(outer)[:, None] * (np.arange(128)[None, :] % outer)
    small = 2.0 * np.pi * (a % outer) / outer
    b = np.arange(inner)[:, None] * np.arange(size)[None, :]
    big = 2.0 * np.pi * (b % size) / size
    waves = [np.concatenate([f(small), f(big) / size], axis=1) for f in (np.cos, np.sin)]
    return np.concatenate(waves, axis=0).astype(np.float32)


def build_pair_table(rate_ref, wide_ref, table_ref):
    nodes = rate_ref.shape[0]
    half = nodes // 2
    g, _ = pair_constants(nodes)
    wide_ref[...] = rate_ref[...].astype(jnp.float32)
    for k in range(half):
        a = wide_ref[k : k + 1, :]
        b = wide_ref[nodes - 1 - k : nodes - k, :]
        table_ref[k : k + 1, :] = a + b
        table_ref[half + k : half + k + 1, :] = a * np.float32(1.0 / g[k]) + b * np.float32(g[k])


def build_rows(tiles_ref, rows_ref):
    tiles_x, tiles_y, tiles_z = tiles_ref.shape
    group = lax.broadcasted_iota(jnp.int32, (1, 128), 1) // EDGE
    for b in range(tiles_y):
        for t in range(tiles_z):
            row = jnp.zeros((1, 128), jnp.int32)
            for a in range(tiles_x):
                value = jnp.broadcast_to(tiles_ref[a, b : b + 1, t : t + 1], (1, 128))
                row = jnp.where(group == a, value, row)
            i = b * tiles_z + t
            rows_ref[i : i + 1, :] = row


def column_integral(field, index_row, table_ref, coef_ref):
    nodes = table_ref.shape[0]
    half = nodes // 2
    _, s = pair_constants(nodes)
    index = jnp.broadcast_to(index_row, (8, 128))
    for part in range(nodes // 8):
        rows = pl.ds(8 * part, 8)
        coef_ref[rows, :] = jnp.take_along_axis(
            table_ref[rows, :], index, axis=1, mode="promise_in_bounds"
        )
    w = jnp.exp(3.0 * field)
    v = w + jnp.exp(-3.0 * field)
    total = jnp.zeros_like(field)
    for k in range(half):
        r = pl.reciprocal(v + np.float32(s[k]), approx=False)
        total = total + (w * coef_ref[k : k + 1, :] + coef_ref[half + k : half + k + 1, :]) * r
    return total


def split(x):
    high = x.astype(jnp.bfloat16)
    return high, (x - high.astype(jnp.float32)).astype(jnp.bfloat16)


def window_rows(filt, wave_ref):
    flipped = jnp.transpose(filt)
    real = jnp.zeros((32, 128), jnp.float32)
    imag = jnp.zeros((32, 128), jnp.float32)
    for a in range(32):
        r, q = a // 4, a % 4
        column = jnp.broadcast_to(flipped[32 * q : 32 * q + 32, r : r + 1], (32, 128))
        real = real + column * wave_ref[a : a + 1, :128]
        imag = imag + column * wave_ref[32 + a : 33 + a, :128]
    rows = []
    for m in range(8):
        lanes = pl.ds(128 * (m + 1), 128)
        value = real * wave_ref[0:32, lanes] - imag * wave_ref[32:64, lanes]
        rows.append(jnp.sum(value, axis=0, keepdims=True))
    return rows


def build_circulant(rows, store):
    lane = lax.broadcasted_iota(jnp.int32, (128, 128), 1)
    down = lax.broadcasted_iota(jnp.int32, (128, 128), 0)
    shift = lax.rem(lane - down + 128, 128)
    upper = lane >= down
    rolled = []
    for m in range(8):
        row = jnp.broadcast_to(rows[m], (8, 128))
        rolled.append(
            jnp.concatenate(
                [
                    jnp.take_along_axis(row, shift[8 * g : 8 * g + 8], axis=1, mode="promise_in_bounds")
                    for g in range(16)
                ],
                axis=0,
            )
        )
    blocks = [jnp.where(upper, rolled[(-d) % 8], rolled[(-d - 1) % 8]) for d in range(8)]
    for d in range(-3, 4):
        near, far = blocks[d % 8], blocks[(d + 4) % 8]
        for sign, value in enumerate((0.5 * (near + far), 0.5 * (near - far))):
            for i in range(4):
                j = i - d
                if 0 <= j < 4:
                    store(sign, i, j, value)


def dot3(a, b):
    d = functools.partial(jnp.dot, preferred_element_type=jnp.float32)
    return d(a[0], b[0]) + d(a[0], b[1]) + d(a[1], b[0])


def fused_kernel(
    field_hbm, bins_hbm, rate_hbm, mask_hbm, route_hbm, fx_hbm, fy_hbm, wave_hbm,
    recomb_ref, smooth_ref, share_ref,
    field_buf, lt_ref, rt_ref, zsend_ref, recv_ref, mx_ref, my_ref, mid_ref, send_ref, back_ref, give_ref,
    bins_ref, rate_ref, mask_tiles, route_tiles, fx_ref, fy_ref, wave_ref, wide_ref, table_ref, mask_ref, route_ref, coef_ref, sum_ref,
    in_sem, small_sem, fsend_sem, frecv_sem, bsend_sem, brecv_sem, lsend_sem, lrecv_sem,
):
    n_gx, n_gy = lax.axis_size("gx"), lax.axis_size("gy")
    total = n_gx * n_gy
    gx, gy = lax.axis_index("gx"), lax.axis_index("gy")
    me = gx * n_gy + gy
    cx, core = gx // 2, lax.rem(gx, 2)
    cy, cz = gy // 4, lax.rem(gy, 4)
    layers = bins_ref.shape[1]
    chunks = zsend_ref.shape[0]
    pieces = send_ref.shape[0]
    tile = lax.rem(cx + cy + cz, 4)
    plane = tile * EDGE + gx * 4 + cy
    xs = [lax.rem(cx + e, 4) for e in range(4)]
    ys = [lax.rem(cy + b, 4) for b in range(4)]
    tys = [lax.rem(gy + j, n_gy) for j in range(n_gy)]

    def fetch(c, slot):
        return pltpu.make_async_copy(
            field_hbm.at[:, pl.ds(pl.multiple_of(c * 8, 8), 8), :], field_buf.at[slot], in_sem.at[slot]
        )

    small = [
        pltpu.make_async_copy(source, target, small_sem.at[i])
        for i, (source, target) in enumerate(
            (
                (rate_hbm, rate_ref), (mask_hbm, mask_tiles), (bins_hbm, bins_ref),
                (route_hbm, route_tiles), (fx_hbm, fx_ref), (fy_hbm, fy_ref), (wave_hbm, wave_ref),
            )
        )
    ]
    fetch(0, 0).start()
    for copy in small:
        copy.start()
    barrier = pltpu.get_barrier_semaphore()

    def greet(i, _):
        tx = lax.rem(gx + i, n_gx)
        for j in range(1, n_gy):
            pl.semaphore_signal(barrier, inc=1, device_id=(tx, tys[j]), device_id_type=MESH)

        @pl.when(i > 0)
        def _():
            pl.semaphore_signal(barrier, inc=1, device_id=(tx, gy), device_id_type=MESH)

        return 0

    lax.fori_loop(0, n_gx, greet, 0)
    small[0].wait()
    build_pair_table(rate_ref, wide_ref, table_ref)
    small[1].wait()
    build_rows(mask_tiles, mask_ref)
    small[2].wait()
    sum_ref[...] = jnp.zeros_like(sum_ref)

    def forward(c, t, side, zs, e, b):
        tx = xs[e] * 2 + side
        ty = ys[b] * 4 + zs[(e + b) % 4]
        return pltpu.make_async_remote_copy(
            src_ref=zsend_ref.at[c, t * EDGE + tx * 4 + ys[b]], dst_ref=recv_ref.at[c, me],
            send_sem=fsend_sem.at[c], recv_sem=frecv_sem.at[c],
            device_id=(tx, ty), device_id_type=MESH,
        )

    def send_unit(c, t, half):
        zs = [lax.rem(t - cx - cy - m + 16, 4) for m in range(4)]
        side = lax.rem(core + half, 2)
        for e in range(4):
            for b in range(4):
                if e + b > 0:
                    forward(c, t, side, zs, e, b).start()

        @pl.when(jnp.logical_or(half > 0, t != tile))
        def _():
            forward(c, t, side, zs, 0, 0).start()

    def evaluate_unit(u, sending):
        c = u // layers
        t = lax.rem(u, layers)
        slot = lax.rem(c, 2)
        band = c * 8 // EDGE
        before = u - 1

        @pl.when(t == 0)
        def _():
            @pl.when(c + 1 < chunks)
            def _():
                fetch(c + 1, 1 - slot).start()

            fetch(c, slot).wait()
            field2 = field_buf.at[slot].reshape(128 * 8, 128)
            for y in range(8):
                lt_ref[y] = field2[pl.ds(y, 128, stride=8), :].T

        zsend2 = zsend_ref.at[c].reshape(128 * 8, 128)
        z = pl.ds(pl.multiple_of(EDGE * t, EDGE), EDGE)
        row = band * layers + t

        def half_rows(half, _):
            if sending:
                send_unit(before // layers, lax.rem(before, layers), half)
            sums = jnp.zeros((8, 128), jnp.float32)
            mask = (mask_ref[pl.ds(row, 1), :] == 1).astype(jnp.float32)
            for i in range(4):
                y = half * 4 + i
                value = column_integral(
                    lt_ref[y, z, :], bins_ref[c * 8 + y, pl.ds(t, 1), :], table_ref, coef_ref.at[i]
                )
                value = value * mask
                rt_ref[y, z, :] = value
                zsend2[pl.ds(t * EDGE * 8 + y, EDGE, stride=8), :] = value
                sums = sums + ((value[0:8] + value[8:16]) + (value[16:24] + value[24:32]))
            sum_ref[row] += sums
            return 0

        lax.fori_loop(0, 2, half_rows, 0)

        @pl.when(t == layers - 1)
        def _():
            out2 = recomb_ref.at[c].reshape(128 * 8, 128)
            for y in range(8):
                out2[pl.ds(y, 128, stride=8), :] = rt_ref[y].T
            recv_ref[c, me] = zsend_ref[c, plane]

    evaluate_unit(0, False)
    pl.semaphore_wait(barrier, total - 1)

    def later_unit(u, _):
        evaluate_unit(u, True)
        return 0

    lax.fori_loop(1, chunks * layers, later_unit, 0)

    def last_unit(half, _):
        send_unit(chunks - 1, layers - 1, half)
        return 0

    lax.fori_loop(0, 2, last_unit, 0)

    small[3].wait()
    build_rows(route_tiles, route_ref)
    flat = jnp.concatenate(
        [jnp.sum(sum_ref[i], axis=0, keepdims=True) for i in range(8)], axis=0
    )
    for g in range(16):
        give_ref[g] = jnp.where(route_ref[...] == g, flat, 0.0)
    share_ref[gy] = give_ref[gy]

    for copy in small[4:]:
        copy.wait()

    def store_x(sign, i, j, value):
        for part, piece in enumerate(split(value)):
            mx_ref[sign, part, pl.ds(128 * i, 128), pl.ds(128 * j, 128)] = piece

    def store_y(sign, i, j, value):
        order = jnp.concatenate(
            [value[64 * h + 8 * p : 64 * h + 8 * p + 8] for p in range(8) for h in range(2)], axis=0
        )
        for part, piece in enumerate(split(order)):
            for p in range(8):
                my_ref[sign, part, p, pl.ds(16 * i, 16), pl.ds(128 * j, 128)] = piece[16 * p : 16 * p + 16]

    build_circulant(window_rows(fx_ref[...], wave_ref), store_x)
    build_circulant(window_rows(fy_ref[...], wave_ref), store_y)

    def load_copy(k):
        ty = lax.rem(gy + k, n_gy)
        return pltpu.make_async_remote_copy(
            src_ref=give_ref.at[ty], dst_ref=share_ref.at[gy],
            send_sem=lsend_sem, recv_sem=lrecv_sem,
            device_id=(gx, ty), device_id_type=MESH,
        )

    def load_send(k, _):
        load_copy(k).start()
        return 0

    lax.fori_loop(1, n_gy, load_send, 0)

    def wait_all(ref, send_sem, recv_sem, what):
        copy = pltpu.make_async_remote_copy(
            src_ref=ref, dst_ref=ref, send_sem=send_sem, recv_sem=recv_sem,
            device_id=(gx, gy), device_id_type=MESH,
        )
        copy.wait_recv() if what == "recv" else copy.wait_send()

    def first(c, _):
        for q in range(2):
            wait_all(recv_ref.at[2 * c + q, pl.ds(0, total - 1)], fsend_sem.at[2 * c + q], frecv_sem.at[2 * c + q], "recv")

        def rows(i, j0):
            src = pl.ds(i * 16 + j0, 8)
            return jnp.concatenate([recv_ref[2 * c, src], recv_ref[2 * c + 1, src]], axis=1).reshape(128, 128)

        for ysign in range(2):
            parts = [[], []]
            for i in range(4):
                a0, a1 = rows(i, 0), rows(i, 8)
                b0, b1 = rows(i + 4, 0), rows(i + 4, 8)
                if ysign == 0:
                    a, b = a0 + a1, b0 + b1
                else:
                    a, b = a0 - a1, b0 - b1
                parts[0].append(a + b)
                parts[1].append(a - b)
            for xsign in range(2):
                value = split(jnp.concatenate(parts[xsign], axis=1))
                out = split(dot3(value, (mx_ref[xsign, 0], mx_ref[xsign, 1])))
                for part in range(2):
                    for j in range(8):
                        mid_ref[ysign, part, pl.ds(pl.multiple_of(64 * j + 16 * c, 16), 16), pl.ds(512 * xsign, 512)] = out[part][16 * j : 16 * j + 16]
        return 0

    lax.fori_loop(0, chunks // 2, first, 0)

    def backward(p, tx, ty):
        return pltpu.make_async_remote_copy(
            src_ref=send_ref.at[p, tx * n_gy + ty], dst_ref=back_ref.at[p, plane],
            send_sem=bsend_sem.at[p], recv_sem=brecv_sem.at[p],
            device_id=(tx, ty), device_id_type=MESH,
        )

    def second(p, _):
        res = [
            dot3((my_ref[ysign, 0, p], my_ref[ysign, 1, p]), (mid_ref[ysign, 0], mid_ref[ysign, 1]))
            for ysign in range(2)
        ]
        for yh in range(2):
            both = res[0] + res[1] if yh == 0 else res[0] - res[1]
            plus, minus = both[:, :512], both[:, 512:]
            for xh in range(2):
                value = plus + minus if xh == 0 else plus - minus
                for i in range(4):
                    for j in range(8):
                        send_ref[p, (xh * 4 + i) * 16 + yh * 8 + j] = value[8 * j : 8 * j + 8, 128 * i : 128 * i + 128]
        back_ref[p, plane] = send_ref[p, me]

        def send(i, _):
            for j in range(1, n_gy):
                backward(p, lax.rem(gx + i + 3 * j, n_gx), tys[j]).start()

            @pl.when(i > 0)
            def _():
                backward(p, lax.rem(gx + i, n_gx), gy).start()

            return 0

        lax.fori_loop(0, n_gx, send, 0)
        return 0

    lax.fori_loop(0, pieces, second, 0)

    def finish_forward(c, _):
        wait_all(zsend_ref.at[c, pl.ds(0, total - 1)], fsend_sem.at[c], frecv_sem.at[c], "send")
        return 0

    lax.fori_loop(0, chunks, finish_forward, 0)
    wait_all(share_ref.at[pl.ds(0, n_gy - 1)], lsend_sem, lrecv_sem, "recv")
    wait_all(give_ref.at[pl.ds(0, n_gy - 1)], lsend_sem, lrecv_sem, "send")

    def finish_backward(p, _):
        wait_all(back_ref.at[p, pl.ds(0, total - 1)], bsend_sem.at[p], brecv_sem.at[p], "recv")
        source = back_ref.at[p].reshape(128 * 8, 128)
        target = smooth_ref.at[p].reshape(128 * 8, 128)
        for y in range(8):
            target[pl.ds(y, 128, stride=8), :] = source[pl.ds(y, 128, stride=8), :].T
        wait_all(send_ref.at[p, pl.ds(0, total - 1)], bsend_sem.at[p], brecv_sem.at[p], "send")
        return 0

    lax.fori_loop(0, pieces, finish_backward, 0)


def fused_call(log_crit, bins, rate, tile_mask, tile_route, fx, fy):
    f32, bf16, i32 = jnp.float32, jnp.bfloat16, jnp.int32
    cells_x, cells_y, depth = log_crit.shape
    total = lax.axis_size("gx") * lax.axis_size("gy")
    chunks = cells_y // 8
    waves = wave_tables(fx.size)
    dma = pltpu.SemaphoreType.DMA
    vmem, hbm = pl.BlockSpec(memory_space=VMEM), pl.BlockSpec(memory_space=pltpu.HBM)
    blocks = jax.ShapeDtypeStruct((chunks, cells_x, 8, depth), f32)
    return pl.pallas_call(
        fused_kernel,
        in_specs=[hbm] * 8,
        out_specs=[vmem, vmem, vmem],
        out_shape=[blocks, blocks, jax.ShapeDtypeStruct((16, 8, 128), f32)],
        scratch_shapes=[
            VMEM((2, cells_x, 8, depth), f32),
            VMEM((8, 128, 128), f32),
            VMEM((8, 128, 128), f32),
            VMEM((chunks, total, 8, 128), f32),
            VMEM((chunks, total, 8, 128), f32),
            VMEM((2, 2, 512, 512), bf16),
            VMEM((2, 2, 8, 64, 512), bf16),
            VMEM((2, 2, 512, 1024), bf16),
            VMEM((chunks, total, 8, 128), f32),
            VMEM((chunks, total, 8, 128), f32),
            VMEM((16, 8, 128), f32),
            VMEM(bins.shape, i32),
            VMEM(rate.shape, bf16),
            VMEM(tile_mask.shape, i32),
            VMEM(tile_route.shape, i32),
            VMEM(fx.shape, f32),
            VMEM(fy.shape, f32),
            VMEM(waves.shape, f32),
            VMEM(rate.shape, f32),
            VMEM(rate.shape, f32),
            VMEM((8, 128), i32),
            VMEM((8, 128), i32),
            VMEM((4, *rate.shape), f32),
            VMEM((8, 8, 128), f32),
            dma((2,)), dma((7,)), dma((chunks,)), dma((chunks,)), dma((chunks,)), dma((chunks,)), dma, dma,
        ],
        compiler_params=pltpu.CompilerParams(
            vmem_limit_bytes=40 * 2**20, collective_id=0, has_side_effects=True
        ),
        name="fused",
    )(*(pltpu.with_memory_space_constraint(a, pltpu.HBM) for a in (log_crit, bins, rate, tile_mask, tile_route, fx, fy, jnp.asarray(waves))))


def final_kernel(recomb_ref, smooth_ref, share_ref, recomb_hbm, smooth_hbm, load_ref, sems):
    copies = []
    for a, (source, target) in enumerate(((recomb_ref, recomb_hbm), (smooth_ref, smooth_hbm))):
        for c in range(source.shape[0]):
            copies.append(pltpu.make_async_copy(source.at[c], target.at[:, pl.ds(8 * c, 8), :], sems.at[a, c]))
    for copy in copies:
        copy.start()
    shares = jnp.sum(share_ref[...], axis=0)
    load_ref[...] = jnp.sum(jnp.sum(shares, axis=0, keepdims=True), axis=1, keepdims=True) * (2.0**-19)
    for copy in copies:
        copy.wait()


def final_call(recomb, smooth, share):
    chunks, cells_x, rows, depth = recomb.shape
    f32 = jnp.float32
    whole = jax.ShapeDtypeStruct((cells_x, chunks * rows, depth), f32)
    vmem, anywhere = pl.BlockSpec(memory_space=VMEM), pl.BlockSpec(memory_space=pl.ANY)
    return pl.pallas_call(
        final_kernel,
        in_specs=[vmem] * 3,
        out_specs=[anywhere, anywhere, vmem],
        out_shape=[whole, whole, jax.ShapeDtypeStruct((1, 1), f32)],
        scratch_shapes=[pltpu.SemaphoreType.DMA((2, chunks))],
        compiler_params=pltpu.CompilerParams(vmem_limit_bytes=16 * 2**20),
        name="final",
    )(recomb, smooth, share)


def on_device(log_crit, col_bins, rate_table, tile_mask, tile_route, filt_x, filt_y):
    recomb, smooth, share = fused_call(
        log_crit, col_bins.transpose(1, 2, 0), rate_table.T, tile_mask, tile_route,
        filt_x.reshape(-1, 128), filt_y.reshape(-1, 128),
    )
    recomb, smooth, load = final_call(recomb, smooth, share)
    return recomb, smooth, load


def solution(mesh):
    block = P("gx", "gy", None)
    return jax.shard_map(
        on_device,
        mesh=mesh,
        in_specs=(block, block, P(), block, block, P(), P()),
        out_specs=(block, block, P("gx", "gy")),
        check_vma=False,
    )
```
